1024 devices in a mesh: section: 16 (over z_hi, y, core), dp: 64 (over z_lo, x).
Axes of the slice: x: 4, y: 4, z: 32 (z_hi: 2, z_lo: 16; z = z_hi * 16 + z_lo), core: 2. Of those that a mesh axis runs over, the one named last changes fastest.
Arguments:
- tokens: bfloat16 [512, 6144], P('dp', 'section'), may hold values from -6 to 6
- expert_ids: int32 [512, 2], P('dp'), may hold values from 0 to 7, all different within a row; in each aligned block of 8 rows (0 to 7, 8 to 15, ...) at most 4 rows name the same one
- router: bfloat16 [6144, 8], replicated, may hold values from -0.078125 to 0.078125
- w_up: bfloat16 [64, 6144, 2048], P('dp', None, 'section'), may hold values from -0.078125 to 0.078125
- w_down: bfloat16 [64, 2048, 6144], P('dp', 'section'), may hold values from -0.0625 to 0.0625
- attn_queries: bfloat16 [64, 128, 6144], P('dp', None, 'section'), may hold values from -140 to 140
- attn_keys: bfloat16 [64, 128, 6144], P('dp', None, 'section'), may hold values from -8 to 8
- attn_values: bfloat16 [64, 128, 6144], P('dp', None, 'section'), may hold values from -6 to 6
Outputs:
- mixed: bfloat16 [512, 6144], P('dp', 'section')
- attended: bfloat16 [64, 128, 6144], P('dp', None, 'section')
The draws below stay inside these ranges and needn't reach their ends.
Inputs may be any that keep to these rules, and one draw needn't show every extreme that they name: `expert_ids`: each row names two different experts; among the 8 rows of one dp index (aligned blocks) no expert is named more than 4 times.
All inputs are finite; a program needn't handle non-finite values.
Results may differ from the reference program's by a relative error of at most 0.005.
Values may be sent and summed in bfloat16 or wider, within the bound.
A program may use at most 32 MiB of HBM per device.

```python
import math
import jax
import jax.numpy as jnp
import numpy as np
from jax import lax

D = 6144
FF = 16384
EXPERTS = 8
ATT_HEADS = 48
HEAD_DIM = 128
CAP = 4
TOK_DP = 8
SEQ = 128
RSPLIT = 8
TOKENS = 512
N_DP = 64


def attention_pair(key):
    base = jax.random.fold_in(key, 7)
    key_query, key_keys = jax.random.split(base, 2)
    shape = (N_DP, SEQ, ATT_HEADS * HEAD_DIM)
    key_array = jnp.clip(jax.random.normal(key_keys, shape, jnp.float32), -6.0, 6.0)
    query_array = jnp.clip(jax.random.normal(key_query, shape, jnp.float32), -6.0, 6.0)
    return (query_array, key_array)


def draw_attn_queries(key, part):
    query_array, key_array = attention_pair(key)
    return query_array.astype(jnp.bfloat16)


def draw_attn_keys(key, part):
    query_array, key_array = attention_pair(key)
    return key_array.astype(jnp.bfloat16)


def raised(result, rng, source, target, shards_of, factor):
    def block_of(position):
        return (jnp.arange(result.shape[position]) // (result.shape[position] // shards_of)).reshape((-1,) + (1,) * (result.ndim - 1 - position))

    near = jax.random.permutation(rng, shards_of)[block_of(target)]
    second = (block_of(target) + shards_of // 2) % shards_of
    return jnp.where((block_of(source) == near) | (block_of(source) == second), factor * result, result)


def levels(stream_key, extent, cuts, smallest, high):
    loudness, own = 1.0, jax.random.fold_in(stream_key, 6)
    for dim, blocks in cuts:
        draws = jnp.exp(jax.random.uniform(jax.random.fold_in(own, dim), (blocks,), jnp.float32, smallest / len(cuts), high / len(cuts)))
        loudness = loudness * jnp.repeat(draws, extent[dim] // blocks).reshape([-1 if axis == dim else 1 for axis in range(len(extent))])
    return loudness


def shared_out(key, own, number, rows, amount, top, limit, skew):
    sequence = jax.random.permutation(key, amount)
    packed, usual = shares(amount, rows * top, limit, skew, True), shares(amount, rows * top, limit, skew, False)
    places = jnp.arange(amount)

    def named(sizes, rotation):
        used = int((sizes > 0).sum())
        fixed = max(1, used // 4)
        passed = fixed + (places - fixed + rotation * (used - fixed)) % max(1, amount - fixed)
        return jnp.zeros((amount,), jnp.int32).at[sequence[jnp.where(places < fixed, places, passed)]].set(jnp.asarray(sizes, jnp.int32))

    sizes = jnp.where(number % 4 == 0, named(packed, number // 4), named(usual, number - number // 4 - 1))
    mixed = jax.random.permutation(jax.random.fold_in(own, 3), amount)
    giver, receiver = mixed[0:amount // 2 * 2:2], mixed[1:amount // 2 * 2:2]
    margin = jnp.minimum(sizes[giver] - 1, limit - sizes[receiver]) // 2
    margin = jnp.where((giver == sequence[0]) | (receiver == sequence[0]) | (sizes[receiver] == 0), 0, jnp.maximum(margin, 0))
    passed = jax.random.randint(jax.random.fold_in(own, 4), (amount // 2,), 0, 1 << 20) % (margin + 1)
    sizes = sizes.at[giver].add(-passed).at[receiver].add(passed)
    labels = jnp.searchsorted(jnp.cumsum(sizes), jnp.arange(rows * top), side="right").astype(jnp.int32)
    grid = labels.reshape(top, rows).T
    grid = grid[jax.random.permutation(jax.random.fold_in(own, 1), rows)]
    rotation = jax.random.randint(jax.random.fold_in(own, 2), (rows, 1), 0, top)
    return jnp.take_along_axis(grid, (jnp.arange(top)[None, :] + rotation) % top, axis=1)


def shares(count, total, limit, skew, full):
    loads = [(1 << 20) // math.isqrt(rank ** skew) + 1 for rank in range(1, count + 1)]
    largest = limit if full else min(limit, max(-(-total // count), total * loads[0] // sum(loads)))
    least = 1 if total - largest >= count - 1 else 0
    given, surplus = [largest] + [least] * (count - 1), total - largest - least * (count - 1)
    while surplus > 0:
        candidates = [i for i in range(1, count) if given[i] < largest] or [i for i in range(1, count) if given[i] < limit]
        mass, left = sum([loads[i] for i in candidates]), surplus
        for i in candidates:
            extra = min(limit - given[i], max(1, left * loads[i] // mass), surplus)
            given[i] = given[i] + extra
            surplus = surplus - extra
    return np.array(given)


def gaussian(stream_key, extent, deviation, most, cuts=(), held_as=jnp.bfloat16):
    entries = deviation * jax.random.normal(stream_key, extent, jnp.float32)
    if cuts:
        entries = entries * levels(stream_key, extent, cuts, -0.22, 0.18)
    return jnp.clip(entries, -most, most).astype(held_as)


def heavy_noise(stream_key, shape, spread, reach, pieces, heavy, held_as=jnp.bfloat16):
    result = spread * jax.random.normal(stream_key, shape, jnp.float32)
    if pieces:
        result = result * levels(stream_key, shape, pieces, -0.22, 0.18)
    return jnp.clip(raised(result, jax.random.fold_in(stream_key, 3), *heavy), -reach, reach).astype(held_as)


def setup_inputs(seed: int = 0) -> dict:
    key_of = jax.random.split(jax.random.key(seed), 9)
    tokens = gaussian(key_of[0], (TOKENS, D), 1.0, 6.0, ((0, 64), (1, 16)))
    expert_ids_keys = jax.random.split(jax.random.fold_in(key_of[1], 1), TOKENS // TOK_DP)
    expert_ids_turns = jax.random.permutation(jax.random.fold_in(key_of[1], 3), TOKENS // TOK_DP)
    expert_ids = jax.vmap(lambda own, number: shared_out(jax.random.fold_in(key_of[1], 2), own, number, TOK_DP, EXPERTS, 2, CAP, 2))(expert_ids_keys, expert_ids_turns).reshape((TOKENS, 2))
    router = gaussian(key_of[2], (D, EXPERTS), D ** -0.5, 0.078125)
    w_up = gaussian(key_of[3], (N_DP, D, FF // RSPLIT), D ** -0.5, 0.078125, ((0, 64), (2, 16)))
    w_down = heavy_noise(key_of[4], (N_DP, FF // RSPLIT, D), FF ** -0.5, 0.0625, ((0, 64), (1, 16)), (1, 2, 16, 2.0))
    attn_queries = draw_attn_queries(jax.random.fold_in(key_of[8], 71), 0)
    attn_keys = draw_attn_keys(jax.random.fold_in(key_of[8], 71), 0)
    attn_values = gaussian(key_of[7], (N_DP, SEQ, ATT_HEADS * HEAD_DIM), 1.0, 6.0, ((0, 64), (2, 16)))
    return dict(tokens=tokens, expert_ids=expert_ids, router=router, w_up=w_up, w_down=w_down, attn_queries=attn_queries, attn_keys=attn_keys, attn_values=attn_values)


def pair_weights(tokens, router, expert_ids):
    logits = jnp.dot(tokens, router, preferred_element_type=jnp.float32)
    experts = router.shape[1]
    onehot = (expert_ids[:, :, None] == jnp.arange(experts, dtype=jnp.int32)[None, None, :]).astype(jnp.float32)
    chosen = lax.optimization_barrier(jnp.sum(logits[:, None, :] * onehot, axis=2))
    first_prob = jax.nn.sigmoid(chosen[:, 0] - chosen[:, 1])
    return jnp.stack([first_prob, 1.0 - first_prob], axis=1)

def route_slots(expert_ids, block_count, per_block, experts):
    pair_ids = expert_ids.reshape(block_count, per_block * 2)
    onehot = (pair_ids[:, :, None] == jnp.arange(experts, dtype=jnp.int32)[None, None, :]).astype(jnp.int32)
    before = jnp.cumsum(onehot, axis=1) - onehot
    slot_rank = lax.optimization_barrier(jnp.sum(before * onehot, axis=2))
    return slot_rank.reshape(block_count * per_block, 2)

def attend_head(operands):
    head_queries, head_keys, head_values = operands
    length = head_queries.shape[0]
    scores = jnp.dot(head_queries, head_keys.T, preferred_element_type=jnp.float32) * (1.0 / math.sqrt(head_queries.shape[1]))
    positions = jnp.arange(length, dtype=jnp.int32)
    causal = positions[None, :] <= positions[:, None]
    scores = jnp.where(causal, scores, -jnp.inf)
    row_max = lax.optimization_barrier(jnp.max(scores, axis=1, keepdims=True))
    exp_scores = jnp.exp(scores - row_max)
    row_total = lax.optimization_barrier(jnp.sum(exp_scores, axis=1, keepdims=True))
    probs = (exp_scores / row_total).astype(jnp.bfloat16)
    return jnp.dot(probs, head_values, preferred_element_type=jnp.float32).astype(jnp.bfloat16)

def attention(attn_queries, attn_keys, attn_values):
    batch, length, width = attn_queries.shape
    heads = width // HEAD_DIM

    def split_heads(array):
        return jnp.transpose(array.reshape(batch, length, heads, HEAD_DIM), (0, 2, 1, 3)).reshape(batch * heads, length, HEAD_DIM)
    outputs = lax.map(attend_head, (split_heads(attn_queries), split_heads(attn_keys), split_heads(attn_values)))
    return jnp.transpose(outputs.reshape(batch, heads, length, HEAD_DIM), (0, 2, 1, 3)).reshape(batch, length, width)

def reference(tokens, expert_ids, router, w_up, w_down, attn_queries, attn_keys, attn_values):
    token_count, model_width = tokens.shape
    experts = router.shape[1]
    block_count = w_up.shape[0]
    split_count = block_count // experts
    per_block = token_count // block_count
    slot_count = block_count * CAP
    pair_prob = pair_weights(tokens, router, expert_ids)
    slot_rank = route_slots(expert_ids, block_count, per_block, experts)
    block_of = (jnp.arange(token_count, dtype=jnp.int32) // per_block)[:, None]
    slot_of = block_of * CAP + slot_rank
    slot_range = jnp.arange(slot_count, dtype=jnp.int32)
    token_rows = tokens.astype(jnp.float32)

    def one_expert(carried, expert):
        chosen_here = expert_ids == expert
        matched = (slot_of[:, :, None] == slot_range[None, None, :]) & chosen_here[:, :, None]
        selector = jnp.any(matched, axis=1).astype(jnp.float32)
        weighting = lax.optimization_barrier(jnp.sum(matched.astype(jnp.float32) * pair_prob[:, :, None], axis=1))
        rows = jnp.dot(selector.T, token_rows, precision=lax.Precision.HIGHEST).astype(jnp.bfloat16)
        first = (expert * split_count).astype(jnp.int32)
        up_part = lax.dynamic_slice_in_dim(w_up, first, split_count, 0)
        up_full = jnp.transpose(up_part, (1, 0, 2)).reshape(model_width, -1)
        down_full = lax.dynamic_slice_in_dim(w_down, first, split_count, 0).reshape(-1, model_width)
        activated = jax.nn.silu(jnp.dot(rows, up_full, preferred_element_type=jnp.float32)).astype(jnp.bfloat16)
        expert_out = jnp.dot(activated, down_full, preferred_element_type=jnp.float32)
        return (carried + jnp.dot(weighting, expert_out, precision=lax.Precision.HIGHEST), None)
    summed, _ = lax.scan(one_expert, jnp.zeros((token_count, model_width), jnp.float32), jnp.arange(experts, dtype=jnp.int32))
    attended = attention(attn_queries, attn_keys, attn_values)
    return (summed.astype(jnp.bfloat16), attended)
```

```python
import functools
import math

import jax
import jax.numpy as jnp
from jax import lax
from jax.experimental import pallas as pl
from jax.experimental.pallas import tpu as pltpu
from jax.sharding import PartitionSpec as P

HEAD_DIM = 128
CAP = 4
WIDTH = 384
HIDDEN = 128
MESH = pl.DeviceIdType.MESH
F32, BF16 = jnp.float32, jnp.bfloat16

ORDER = (0, 1, 3, 2)
FAR_FIRST = (8, 7, 9, 6, 10, 5, 11, 4, 12, 3, 13, 2, 14, 1, 15)


def kernel(
    tok_ref, ids_ref, router_ref, up_ref, down_ref, q_hbm, k_hbm, v_hbm,
    mixed_ref, att_ref,
    q_ref, k_ref, v_ref, router_vm, w_up, w_down,
    rows32, pieces, z_in, x_all, h_own, h_in, act, o_all,
    r1, s1, r2, s2, r3, half16, z_out, z_back, gathered,
    logit_own, logit_far, logit_half, logit_in, logit_sum, logit_pair,
    load_sem, wu_sem, wd_sem,
    zs_sem, zr_sem,
    zp_s, zp_r, i_s, i_r, j_s, j_r, h_s, h_r,
    a_s, a_r, b_s, b_r, p_s, p_r, f_s, f_r,
    l_s, l_r,
):
    sec, dp = lax.axis_index("section"), lax.axis_index("dp")
    c = sec % 2
    y = (sec // 2) % 4
    h = sec // 8
    x = dp % 4
    zl = dp // 4
    p = zl % 2
    e = zl // 2
    z = h * 16 + zl
    b0 = z // 8
    i = x * (1 - c) + y * c
    j = y * (1 - c) + x * c

    def dev(x_, y_, z_, c_):
        return {"section": ((z_ // 16) * 4 + y_) * 2 + c_, "dp": (z_ % 16) * 4 + x_}

    def i_peer(d):
        return dev((x + d * (1 - c)) % 4, (y + d * c) % 4, z, c)

    def j_peer(d):
        return dev((x + d * c) % 4, (y + d * (1 - c)) % 4, z, c)

    partner = dev(x, y, z, 1 - c)
    z_pair = dev(x, y, z + 1 - 2 * p, c)
    z_opp = (z + 16) % 32

    def remote(src, dst, s, r, to):
        return pltpu.make_async_remote_copy(
            src_ref=src, dst_ref=dst, send_sem=s, recv_sem=r, device_id=to, device_id_type=MESH
        )

    def drain(ref, sem):
        pltpu.make_async_copy(ref, ref, sem).wait()

    barrier = pltpu.get_barrier_semaphore()
    peers = [dev(x, y, (z + 2 * m) % 32, c) for m in FAR_FIRST]
    peers += [i_peer(d) for d in (1, 2, 3)] + [j_peer(d) for d in (1, 2, 3)] + [z_pair, partner]
    for peer in peers:
        pl.semaphore_signal(barrier, inc=1, device_id=peer, device_id_type=MESH)

    loads = [
        pltpu.make_async_copy(router_ref.at[:, pl.ds(pl.multiple_of(sec * WIDTH, 128), WIDTH)], router_vm, load_sem.at[0]),
        pltpu.make_async_copy(q_hbm, q_ref, load_sem.at[1]),
        pltpu.make_async_copy(k_hbm, k_ref, load_sem.at[2]),
        pltpu.make_async_copy(v_hbm, v_ref, load_sem.at[3]),
    ]
    my_half = pl.ds(pl.multiple_of(c * HIDDEN, HIDDEN), HIDDEN)
    load_up = pltpu.make_async_copy(up_ref.at[:, c], w_up.at[:, :, my_half], wu_sem.at[0])
    for load in loads:
        load.start()
    load_up.start()

    def down_cols(block, core):
        start = pl.multiple_of((block * 2 + core) * WIDTH, 128)
        return down_ref.at[:, pl.ds(start, WIDTH)]

    for block in range(8):
        pltpu.make_async_copy(down_cols(block, c), w_down.at[block, my_half], wd_sem.at[0]).start()

    lane = lax.broadcasted_iota(jnp.int32, (32, 8), 1)
    row = lax.broadcasted_iota(jnp.int32, (32, 8), 0)
    row_expert = row // CAP
    first = (jnp.broadcast_to(ids_ref[0:1, :], (32, 8)) == row_expert).astype(F32)
    second = (jnp.broadcast_to(ids_ref[1:2, :], (32, 8)) == row_expert).astype(F32)
    hit = first + second
    rank = jnp.zeros((32, 8), F32)
    for t in range(7):
        before = jnp.broadcast_to(hit[:, t : t + 1], (32, 8))
        rank = rank + jnp.where(lane > t, before, 0.0)
    in_slot = jnp.where(rank == (row % CAP).astype(F32), hit, 0.0)
    rows32[...] = jnp.dot(in_slot, tok_ref[...].astype(F32), preferred_element_type=F32)
    for ex in range(8):
        pieces[ex] = rows32[pl.ds(CAP * ex, CAP), :].astype(BF16)
    loads[0].wait()
    logit_own[...] = lax.dot_general(
        router_vm[...], tok_ref[...], (((1,), (1,)), ((), ())), preferred_element_type=F32
    )

    pl.semaphore_wait(barrier, len(peers))

    my_slot = (z // 8) * 4 + (zl % 8) // 2
    for m in FAR_FIRST:
        zt = (z + 2 * m) % 32
        remote(
            pieces.at[(zt % 16) // 2], z_in.at[my_slot], zs_sem, zr_sem.at[b0], dev(x, y, zt, c)
        ).start()
    pltpu.make_async_copy(pieces.at[e], z_in.at[my_slot], zr_sem.at[b0]).start()
    remote(logit_own, logit_far, l_s.at[0], l_r.at[0], dev(x, y, z_opp, c)).start()

    send_up = remote(up_ref.at[:, 1 - c], w_up.at[:, :, my_half], wu_sem.at[1], wu_sem.at[2], partner)
    send_up.start()
    for block in range(8):
        remote(
            down_cols(block, 1 - c), w_down.at[block, my_half], wd_sem.at[1], wd_sem.at[2], partner
        ).start()

    for load in loads[1:]:
        load.wait()
    causal = lax.broadcasted_iota(jnp.int32, (128, 128), 1) <= lax.broadcasted_iota(jnp.int32, (128, 128), 0)
    for head in range(3):
        cols = slice(head * HEAD_DIM, (head + 1) * HEAD_DIM)
        scores = lax.dot_general(
            q_ref[:, cols], k_ref[:, cols], (((1,), (1,)), ((), ())), preferred_element_type=F32
        ) * (1.0 / math.sqrt(HEAD_DIM))
        scores = jnp.where(causal, scores, -jnp.inf)
        exp_scores = jnp.exp(scores - jnp.max(scores, axis=1, keepdims=True))
        probs = (exp_scores / jnp.sum(exp_scores, axis=1, keepdims=True)).astype(BF16)
        att_ref[:, cols] = jnp.dot(probs, v_ref[:, cols], preferred_element_type=F32).astype(BF16)

    blocks = [(b0 + o) % 4 for o in ORDER]
    mine16 = pl.ds(pl.multiple_of(p * 16, 16), 16)
    other16 = pl.ds(pl.multiple_of((1 - p) * 16, 16), 16)

    def from_z(k):
        b = blocks[k]
        drain(z_in.at[pl.ds(b * 4, 4)], zr_sem.at[b])
        for s in range(4):
            half16[pl.ds(CAP * s, CAP), :] = z_in[b * 4 + s].astype(F32)
        x_all[k, i, j, mine16, :] = half16[...].astype(BF16)
        strip = x_all.at[k, i, j, mine16]
        remote(strip, strip, zp_s.at[k], zp_r.at[k], z_pair).start()

    def from_pair(k):
        drain(x_all.at[k, i, j, other16], zp_r.at[k])
        tile = x_all.at[k, i, j]
        for d in (1, 2, 3):
            remote(tile, tile, i_s.at[k], i_r.at[k], i_peer(d)).start()

    def from_i(k):
        drain(x_all.at[k, 0, pl.ds(0, 3)], i_r.at[k])
        strip = x_all.at[k, :, j]
        for d in (1, 2, 3):
            remote(strip, strip, j_s.at[k], j_r.at[k], j_peer(d)).start()

    def up(k):
        drain(x_all.at[k, pl.ds(0, 3)], j_r.at[k])
        half = blocks[k] // 2
        total = None
        for ys in range(4):
            left = jnp.concatenate(
                [x_all[k, xs * (1 - c) + ys * c, ys * (1 - c) + xs * c] for xs in range(4)], axis=0
            )
            term = jnp.dot(left, w_up[half * 4 + ys], preferred_element_type=F32)
            total = term if total is None else total + term
        return total

    def swap_hidden(g, total):
        h_own[g] = total
        remote(h_own.at[g], h_in.at[g], h_s.at[g], h_r.at[g], partner).start()

    def activate(g):
        drain(h_in.at[g], h_r.at[g])
        v = h_own[g] + h_in[g]
        act[g] = (v / (1.0 + jnp.exp(-v))).astype(BF16)

    def down(k, g):
        half = blocks[k] // 2
        for yd in range(4):
            out = jnp.dot(act[g], w_down[half * 4 + yd], preferred_element_type=F32).astype(BF16)
            for xd in range(4):
                o_all[k, xd * (1 - c) + yd * c, yd * (1 - c) + xd * c] = out[xd * 32 : (xd + 1) * 32]
        for d in (2, 1, 3):
            remote(
                o_all.at[k, :, (j + d) % 4], r1.at[k, d - 1], a_s.at[k], a_r.at[k], j_peer(d)
            ).start()

    def sum_j(k):
        drain(r1.at[k], a_r.at[k])
        for n in range(4):
            s1[k, n] = (
                o_all[k, n, j].astype(F32)
                + r1[k, 0, n].astype(F32)
                + r1[k, 1, n].astype(F32)
                + r1[k, 2, n].astype(F32)
            ).astype(BF16)
        for d in (2, 1, 3):
            remote(s1.at[k, (i + d) % 4], r2.at[k, d - 1], b_s.at[k], b_r.at[k], i_peer(d)).start()

    def sum_i(k):
        drain(r2.at[k], b_r.at[k])
        s2[k] = (
            s1[k, i].astype(F32)
            + r2[k, 0].astype(F32)
            + r2[k, 1].astype(F32)
            + r2[k, 2].astype(F32)
        )
        remote(s2.at[k, other16], r3.at[k], p_s.at[k], p_r.at[k], z_pair).start()

    def sum_pair(k):
        drain(r3.at[k], p_r.at[k])
        half16[...] = s2[k, mine16, :] + r3[k]
        for s in range(4):
            z_out[k, s] = half16[pl.ds(CAP * s, CAP), :].astype(BF16)
        b = blocks[k]
        for s in range(4):
            zt = b * 8 + 2 * s + p
            target = z_back.at[h * 8 + e]

            @pl.when(zt != z)
            def _():
                remote(z_out.at[k, s], target, f_s, f_r, dev(x, y, zt, c)).start()

            @pl.when(zt == z)
            def _():
                pltpu.make_async_copy(z_out.at[k, s], target, f_r).start()

    from_z(0)
    from_pair(0)
    from_z(1)
    from_z(2)
    from_i(0)
    from_pair(1)
    from_pair(2)
    from_z(3)
    from_i(1)
    from_i(2)
    from_pair(3)

    drain(logit_far, l_r.at[0])
    logit_half[...] = logit_own[...] + logit_far[...]
    for d in (1, 2, 3):
        remote(
            logit_half, logit_in.at[d - 1], l_s.at[1], l_r.at[1], dev(x, (y + d) % 4, z, c)
        ).start()

    load_up.wait()
    send_up.wait_send()
    drain(w_up.at[:, :, pl.ds(0, HIDDEN)], wu_sem.at[2])
    near = up(0)
    from_i(3)
    beside = up(1)
    beside = beside + up(2)
    swap_hidden(1, beside)

    drain(w_down.at[:, pl.ds(0, HIDDEN)], wd_sem.at[0])
    drain(w_down.at[:, pl.ds(0, HIDDEN)], wd_sem.at[1])
    drain(w_down.at[:, pl.ds(0, HIDDEN)], wd_sem.at[2])
    activate(1)
    down(1, 1)
    down(2, 1)
    near = near + up(3)
    swap_hidden(0, near)
    sum_j(1)
    activate(0)
    down(3, 0)
    down(0, 0)
    sum_j(2)
    sum_i(1)
    sum_i(2)
    sum_j(3)
    sum_pair(1)
    sum_pair(2)
    sum_j(0)
    sum_i(3)
    sum_i(0)
    sum_pair(3)
    sum_pair(0)

    drain(logit_in, l_r.at[1])
    logit_sum[...] = logit_half[...] + logit_in[0] + logit_in[1] + logit_in[2]
    remote(logit_sum, logit_pair, l_s.at[2], l_r.at[2], partner).start()
    drain(logit_pair, l_r.at[2])
    full = logit_sum[...] + logit_pair[...]
    named = lax.broadcasted_iota(jnp.int32, (8, 8), 0)
    chosen0 = jnp.sum(jnp.where(named == ids_ref[0:1, :], full, 0.0), axis=0, keepdims=True)
    chosen1 = jnp.sum(jnp.where(named == ids_ref[1:2, :], full, 0.0), axis=0, keepdims=True)
    prob0 = jax.nn.sigmoid(chosen0 - chosen1)
    coefficient = in_slot * (first * prob0 + second * (1.0 - prob0))

    drain(z_back, f_r)
    for ex in range(8):
        gathered[pl.ds(CAP * ex, CAP), :] = z_back[ex].astype(F32) + z_back[8 + ex].astype(F32)
    mixed = lax.dot_general(
        coefficient, gathered[...], (((0,), (0,)), ((), ())), preferred_element_type=F32,
        precision=lax.Precision.HIGHEST,
    )
    mixed_ref[...] = mixed.astype(BF16)

    drain(z_in.at[pl.ds(0, 15)], zs_sem)
    drain(z_back.at[pl.ds(0, 15)], f_s)
    for k in range(4):
        drain(x_all.at[k, 0, 0, pl.ds(0, 16)], zp_s.at[k])
        drain(x_all.at[k, 0, pl.ds(0, 3)], i_s.at[k])
        drain(x_all.at[k, pl.ds(0, 3)], j_s.at[k])
        drain(r1.at[k], a_s.at[k])
        drain(r2.at[k], b_s.at[k])
        drain(r3.at[k], p_s.at[k])
    for g in range(2):
        drain(h_in.at[g], h_s.at[g])
    drain(logit_far, l_s.at[0])
    drain(logit_in, l_s.at[1])
    drain(logit_pair, l_s.at[2])


def per_device(tokens, expert_ids, router, w_up, w_down, attn_queries, attn_keys, attn_values):
    vmem = pl.BlockSpec(memory_space=pltpu.VMEM)
    hbm = pl.BlockSpec(memory_space=pl.ANY)
    dma, one = pltpu.SemaphoreType.DMA, pltpu.SemaphoreType.DMA
    mixed, attended = pl.pallas_call(
        kernel,
        name="window",
        out_shape=(
            jax.ShapeDtypeStruct((8, WIDTH), BF16),
            jax.ShapeDtypeStruct((128, WIDTH), BF16),
        ),
        in_specs=[vmem, vmem, hbm, hbm, hbm, hbm, hbm, hbm],
        out_specs=(vmem, vmem),
        scratch_shapes=[
            pltpu.VMEM((128, WIDTH), BF16),
            pltpu.VMEM((128, WIDTH), BF16),
            pltpu.VMEM((128, WIDTH), BF16),
            pltpu.VMEM((8, WIDTH), BF16),
            pltpu.VMEM((8, WIDTH, 256), BF16),
            pltpu.VMEM((8, 256, WIDTH), BF16),
            pltpu.VMEM((32, WIDTH), F32),
            pltpu.VMEM((8, CAP, WIDTH), BF16),
            pltpu.VMEM((16, CAP, WIDTH), BF16),
            pltpu.VMEM((4, 4, 4, 32, WIDTH), BF16),
            pltpu.VMEM((2, 128, 256), F32),
            pltpu.VMEM((2, 128, 256), F32),
            pltpu.VMEM((2, 128, 256), BF16),
            pltpu.VMEM((4, 4, 4, 32, WIDTH), BF16),
            pltpu.VMEM((4, 3, 4, 32, WIDTH), BF16),
            pltpu.VMEM((4, 4, 32, WIDTH), BF16),
            pltpu.VMEM((4, 3, 32, WIDTH), BF16),
            pltpu.VMEM((4, 32, WIDTH), F32),
            pltpu.VMEM((4, 16, WIDTH), F32),
            pltpu.VMEM((16, WIDTH), F32),
            pltpu.VMEM((4, 4, CAP, WIDTH), BF16),
            pltpu.VMEM((16, CAP, WIDTH), BF16),
            pltpu.VMEM((32, WIDTH), F32),
            pltpu.VMEM((8, 8), F32),
            pltpu.VMEM((8, 8), F32),
            pltpu.VMEM((8, 8), F32),
            pltpu.VMEM((3, 8, 8), F32),
            pltpu.VMEM((8, 8), F32),
            pltpu.VMEM((8, 8), F32),
            dma((4,)), dma((3,)), dma((3,)),
            one, dma((4,)),
            dma((4,)), dma((4,)), dma((4,)), dma((4,)), dma((4,)), dma((4,)), dma((2,)), dma((2,)),
            dma((4,)), dma((4,)), dma((4,)), dma((4,)), dma((4,)), dma((4,)), one, one,
            dma((3,)), dma((3,)),
        ],
        compiler_params=pltpu.CompilerParams(
            collective_id=0, has_side_effects=True, vmem_limit_bytes=67043328
        ),
    )(
        tokens,
        expert_ids.T,
        router.T,
        w_up.reshape(8, 2, WIDTH, HIDDEN),
        w_down.reshape(HIDDEN, 16 * WIDTH),
        attn_queries.reshape(128, WIDTH),
        attn_keys.reshape(128, WIDTH),
        attn_values.reshape(128, WIDTH),
    )
    return mixed, attended.reshape(1, 128, WIDTH)


def solution(mesh):
    placed = (
        P("dp", "section"),
        P("dp", None),
        P(),
        P("dp", None, "section"),
        P("dp", "section", None),
        P("dp", None, "section"),
        P("dp", None, "section"),
        P("dp", None, "section"),
    )
    return jax.shard_map(
        per_device,
        mesh=mesh,
        in_specs=placed,
        out_specs=(P("dp", "section"), P("dp", None, "section")),
        check_vma=False,
    )
```

```python
import functools
import math

import jax
import jax.numpy as jnp
from jax import lax
from jax.experimental import pallas as pl
from jax.experimental.pallas import tpu as pltpu
from jax.sharding import PartitionSpec as P

HEAD_DIM = 128
CAP = 4
WIDTH = 384
HIDDEN = 128
MESH = pl.DeviceIdType.MESH
F32, BF16 = jnp.float32, jnp.bfloat16

DIRECT = (4, -4, 3, -3, 2, -2, 1, -1)


def kernel(
    tok_ref, ids_ref, router_ref, up_ref, down_ref, q_hbm, k_hbm, v_hbm,
    mixed_ref, att_ref,
    q_ref, k_ref, v_ref, router_vm, w_up, w_down,
    rows32, pieces, z_relay, z_in, x_all, h_own, h_in, act, o_all,
    r1, s1, r2, half16, z_out, z_back, gathered,
    logit_own, logit_far, logit_half, logit_in, logit_sum, logit_pair,
    load_sem, wu_sem, wd_sem,
    zs_sem, zr_sem, relay_sem, forward_sem,
    i_s, i_r, j_s, j_r, h_s, h_r,
    a_s, a_r, b_s, b_r, f_s, f_r,
    l_s, l_r,
):
    sec, dp = lax.axis_index("section"), lax.axis_index("dp")
    c = sec % 2
    y = (sec // 2) % 4
    h = sec // 8
    x = dp % 4
    zl = dp // 4
    p = zl % 2
    e = zl // 2
    z = h * 16 + zl
    b0 = z // 8
    i = x * (1 - c) + y * c
    j = y * (1 - c) + x * c

    def dev(x_, y_, z_, c_):
        return {"section": ((z_ // 16) * 4 + y_) * 2 + c_, "dp": (z_ % 16) * 4 + x_}

    def i_peer(d, flip):
        plane = z + flip * (1 - 2 * p)
        return dev((x + d * (1 - c)) % 4, (y + d * c) % 4, plane, c)

    def j_peer(d):
        return dev((x + d * c) % 4, (y + d * (1 - c)) % 4, z, c)

    partner = dev(x, y, z, 1 - c)
    z_opp = (z + 16) % 32

    def remote(src, dst, s, r, to):
        return pltpu.make_async_remote_copy(
            src_ref=src, dst_ref=dst, send_sem=s, recv_sem=r, device_id=to, device_id_type=MESH
        )

    def drain(ref, sem):
        pltpu.make_async_copy(ref, ref, sem).wait()

    barrier = pltpu.get_barrier_semaphore()
    around = [(2, 0), (2, 1), (1, 1), (3, 1), (1, 0), (3, 0), (0, 1)]
    peers = [dev(x, y, (z + 2 * m + 32) % 32, c) for m in DIRECT]
    peers += [i_peer(d, flip) for d, flip in around] + [j_peer(d) for d in (1, 2, 3)] + [partner]
    for peer in peers:
        pl.semaphore_signal(barrier, inc=1, device_id=peer, device_id_type=MESH)

    loads = [
        pltpu.make_async_copy(router_ref.at[:, pl.ds(pl.multiple_of(sec * WIDTH, 128), WIDTH)], router_vm, load_sem.at[0]),
        pltpu.make_async_copy(q_hbm, q_ref, load_sem.at[1]),
        pltpu.make_async_copy(k_hbm, k_ref, load_sem.at[2]),
        pltpu.make_async_copy(v_hbm, v_ref, load_sem.at[3]),
    ]
    my_half = pl.ds(pl.multiple_of(c * HIDDEN, HIDDEN), HIDDEN)
    load_up = pltpu.make_async_copy(up_ref.at[:, c], w_up.at[:, :, my_half], wu_sem.at[0])
    for load in loads:
        load.start()
    load_up.start()

    def down_cols(block, core):
        start = pl.multiple_of((block * 2 + core) * WIDTH, 128)
        return down_ref.at[:, pl.ds(start, WIDTH)]

    for block in range(8):
        pltpu.make_async_copy(down_cols(block, c), w_down.at[block, my_half], wd_sem.at[0]).start()

    lane = lax.broadcasted_iota(jnp.int32, (32, 8), 1)
    row = lax.broadcasted_iota(jnp.int32, (32, 8), 0)
    row_expert = row // CAP
    first = (jnp.broadcast_to(ids_ref[0:1, :], (32, 8)) == row_expert).astype(F32)
    second = (jnp.broadcast_to(ids_ref[1:2, :], (32, 8)) == row_expert).astype(F32)
    hit = first + second
    rank = jnp.zeros((32, 8), F32)
    for t in range(7):
        before = jnp.broadcast_to(hit[:, t : t + 1], (32, 8))
        rank = rank + jnp.where(lane > t, before, 0.0)
    in_slot = jnp.where(rank == (row % CAP).astype(F32), hit, 0.0)
    rows32[...] = jnp.dot(in_slot, tok_ref[...].astype(F32), preferred_element_type=F32)
    for ex in range(8):
        pieces[ex] = rows32[pl.ds(CAP * ex, CAP), :].astype(BF16)
    loads[0].wait()
    logit_own[...] = lax.dot_general(
        router_vm[...], tok_ref[...], (((1,), (1,)), ((), ())), preferred_element_type=F32
    )

    pl.semaphore_wait(barrier, len(peers))

    place = (z % 8) // 2

    def piece_for(m):
        return pieces.at[((z + 2 * m + 32) % 16) // 2]

    up_z, down_z = dev(x, y, (z + 8) % 32, c), dev(x, y, (z + 24) % 32, c)
    for n in (3, 2, 1, 0):
        remote(piece_for(5 + n), z_relay.at[n], zs_sem, relay_sem.at[0], up_z).start()
    for n in (2, 1, 0):
        remote(piece_for(-5 - n), z_relay.at[4 + n], zs_sem, relay_sem.at[1], down_z).start()
    for m in DIRECT:
        remote(
            piece_for(m), z_in.at[b0 * 4 + place], zs_sem, zr_sem.at[b0], dev(x, y, (z + 2 * m + 32) % 32, c)
        ).start()
    pltpu.make_async_copy(pieces.at[e], z_in.at[b0 * 4 + place], zr_sem.at[b0]).start()

    send_up = remote(up_ref.at[:, 1 - c], w_up.at[:, :, my_half], wu_sem.at[1], wu_sem.at[2], partner)
    send_up.start()
    for block in range(8):
        remote(
            down_cols(block, 1 - c), w_down.at[block, my_half], wd_sem.at[1], wd_sem.at[2], partner
        ).start()

    for load in loads[1:]:
        load.wait()
    causal = lax.broadcasted_iota(jnp.int32, (128, 128), 1) <= lax.broadcasted_iota(jnp.int32, (128, 128), 0)
    for head in range(3):
        cols = slice(head * HEAD_DIM, (head + 1) * HEAD_DIM)
        scores = lax.dot_general(
            q_ref[:, cols], k_ref[:, cols], (((1,), (1,)), ((), ())), preferred_element_type=F32
        ) * (1.0 / math.sqrt(HEAD_DIM))
        scores = jnp.where(causal, scores, -jnp.inf)
        exp_scores = jnp.exp(scores - jnp.max(scores, axis=1, keepdims=True))
        probs = (exp_scores / jnp.sum(exp_scores, axis=1, keepdims=True)).astype(BF16)
        att_ref[:, cols] = jnp.dot(probs, v_ref[:, cols], preferred_element_type=F32).astype(BF16)

    mine16 = pl.ds(pl.multiple_of(p * 16, 16), 16)

    def forward():
        drain(z_relay.at[pl.ds(0, 4)], relay_sem.at[0])
        source = (b0 + 3) % 4
        for n in (3, 2, 1, 0):
            remote(
                z_relay.at[n], z_in.at[source * 4 + place], forward_sem, zr_sem.at[source],
                dev(x, y, (z + 2 + 2 * n) % 32, c),
            ).start()
        drain(z_relay.at[pl.ds(0, 3)], relay_sem.at[1])
        source = (b0 + 1) % 4
        for n in (2, 1, 0):
            remote(
                z_relay.at[4 + n], z_in.at[source * 4 + place], forward_sem, zr_sem.at[source],
                dev(x, y, (z + 30 - 2 * n) % 32, c),
            ).start()

    def from_z(b):
        drain(z_in.at[pl.ds(b * 4, 4)], zr_sem.at[b])
        for s in range(4):
            half16[pl.ds(CAP * s, CAP), :] = z_in[b * 4 + s].astype(F32)
        x_all[b, i, j, mine16, :] = half16[...].astype(BF16)
        strip = x_all.at[b, i, j, mine16]
        for d, flip in around:
            remote(strip, strip, i_s.at[b], i_r.at[b], i_peer(d, flip)).start()

    def from_i(b):
        drain(r2.at[b], i_r.at[b])
        strip = x_all.at[b, :, j]
        for d in (2, 1, 3):
            remote(strip, strip, j_s.at[b], j_r.at[b], j_peer(d)).start()

    def up(k):
        drain(x_all.at[k, pl.ds(0, 3)], j_r.at[k])
        half = k // 2
        total = None
        for ys in range(4):
            left = jnp.concatenate(
                [x_all[k, xs * (1 - c) + ys * c, ys * (1 - c) + xs * c] for xs in range(4)], axis=0
            )
            term = jnp.dot(left, w_up[half * 4 + ys], preferred_element_type=F32)
            total = term if total is None else total + term
        return total

    def swap_hidden(g, total):
        h_own[g] = total
        remote(h_own.at[g], h_in.at[g], h_s.at[g], h_r.at[g], partner).start()

    def activate(g):
        drain(h_in.at[g], h_r.at[g])
        v = h_own[g] + h_in[g]
        act[g] = (v / (1.0 + jnp.exp(-v))).astype(BF16)

    def down(k, g):
        half = k // 2
        for yd in range(4):
            out = jnp.dot(act[g], w_down[half * 4 + yd], preferred_element_type=F32).astype(BF16)
            for xd in range(4):
                o_all[k, xd * (1 - c) + yd * c, yd * (1 - c) + xd * c] = out[xd * 32 : (xd + 1) * 32]
        for d in (2, 1, 3):
            remote(
                o_all.at[k, :, (j + d) % 4], r1.at[k, d - 1], a_s.at[k], a_r.at[k], j_peer(d)
            ).start()

    def sum_j(k):
        drain(r1.at[k], a_r.at[k])
        for n in range(4):
            s1[k, n] = (
                o_all[k, n, j].astype(F32)
                + r1[k, 0, n].astype(F32)
                + r1[k, 1, n].astype(F32)
                + r1[k, 2, n].astype(F32)
            ).astype(BF16)
        for d, flip in around:
            rows = pl.ds(pl.multiple_of(((p + flip) % 2) * 16, 16), 16)
            remote(
                s1.at[k, (i + d) % 4, rows], r2.at[k, d * 2 + flip - 1], b_s.at[k], b_r.at[k], i_peer(d, flip)
            ).start()

    def sum_i(k):
        drain(r2.at[k], b_r.at[k])
        total = s1[k, i, mine16, :].astype(F32)
        for n in range(7):
            total = total + r2[k, n].astype(F32)
        half16[...] = total
        for s in range(4):
            z_out[k, s] = half16[pl.ds(CAP * s, CAP), :].astype(BF16)
        for s in range(4):
            zt = k * 8 + 2 * s + p
            target = z_back.at[h * 8 + e]

            @pl.when(zt != z)
            def _():
                remote(z_out.at[k, s], target, f_s, f_r, dev(x, y, zt, c)).start()

            @pl.when(zt == z)
            def _():
                pltpu.make_async_copy(z_out.at[k, s], target, f_r).start()

    odd = b0 % 2
    opposite = (b0 + 2) % 4
    order = [b0, (1 - odd) * opposite, 1 + odd, (1 - odd) * 3 + odd * opposite]
    forward()
    from_z(order[0])
    from_i(order[0])
    from_z(order[1])
    from_z(order[2])
    from_i(order[1])
    from_z(order[3])
    from_i(order[2])
    from_i(order[3])
    remote(logit_own, logit_far, l_s.at[0], l_r.at[0], dev(x, y, z_opp, c)).start()

    load_up.wait()
    send_up.wait_send()
    drain(w_up.at[:, :, pl.ds(0, HIDDEN)], wu_sem.at[2])
    swap_hidden(0, up(0) + up(2))
    drain(w_down.at[:, pl.ds(0, HIDDEN)], wd_sem.at[0])
    drain(w_down.at[:, pl.ds(0, HIDDEN)], wd_sem.at[1])
    drain(w_down.at[:, pl.ds(0, HIDDEN)], wd_sem.at[2])
    activate(0)
    down(0, 0)
    swap_hidden(1, up(1) + up(3))
    sum_j(0)
    activate(1)
    down(1, 1)
    sum_i(0)
    down(2, 0)
    sum_j(1)
    down(3, 1)
    sum_i(1)

    drain(logit_far, l_r.at[0])
    logit_half[...] = logit_own[...] + logit_far[...]
    for d in (1, 2, 3):
        remote(
            logit_half, logit_in.at[d - 1], l_s.at[1], l_r.at[1], dev(x, (y + d) % 4, z, c)
        ).start()
    sum_j(2)
    sum_j(3)
    drain(logit_in, l_r.at[1])
    logit_sum[...] = logit_half[...] + logit_in[0] + logit_in[1] + logit_in[2]
    remote(logit_sum, logit_pair, l_s.at[2], l_r.at[2], partner).start()
    sum_i(2)
    sum_i(3)

    drain(logit_pair, l_r.at[2])
    full = logit_sum[...] + logit_pair[...]
    named = lax.broadcasted_iota(jnp.int32, (8, 8), 0)
    chosen0 = jnp.sum(jnp.where(named == ids_ref[0:1, :], full, 0.0), axis=0, keepdims=True)
    chosen1 = jnp.sum(jnp.where(named == ids_ref[1:2, :], full, 0.0), axis=0, keepdims=True)
    prob0 = jax.nn.sigmoid(chosen0 - chosen1)
    coefficient = in_slot * (first * prob0 + second * (1.0 - prob0))

    drain(z_back, f_r)
    for ex in range(8):
        gathered[pl.ds(CAP * ex, CAP), :] = z_back[ex].astype(F32) + z_back[8 + ex].astype(F32)
    mixed = lax.dot_general(
        coefficient, gathered[...], (((0,), (0,)), ((), ())), preferred_element_type=F32,
        precision=lax.Precision.HIGHEST,
    )
    mixed_ref[...] = mixed.astype(BF16)

    drain(z_in.at[pl.ds(0, 15)], zs_sem)
    drain(z_back.at[pl.ds(0, 15)], f_s)
    drain(z_relay, forward_sem)
    for k in range(4):
        drain(r2.at[k], i_s.at[k])
        drain(r1.at[k], j_s.at[k])
        drain(r1.at[k], a_s.at[k])
        drain(r2.at[k], b_s.at[k])
    for g in range(2):
        drain(h_in.at[g], h_s.at[g])
    drain(logit_far, l_s.at[0])
    drain(logit_in, l_s.at[1])
    drain(logit_pair, l_s.at[2])


def per_device(tokens, expert_ids, router, w_up, w_down, attn_queries, attn_keys, attn_values):
    vmem = pl.BlockSpec(memory_space=pltpu.VMEM)
    hbm = pl.BlockSpec(memory_space=pl.ANY)
    dma, one = pltpu.SemaphoreType.DMA, pltpu.SemaphoreType.DMA
    mixed, attended = pl.pallas_call(
        kernel,
        name="window",
        out_shape=(
            jax.ShapeDtypeStruct((8, WIDTH), BF16),
            jax.ShapeDtypeStruct((128, WIDTH), BF16),
        ),
        in_specs=[vmem, vmem, hbm, hbm, hbm, hbm, hbm, hbm],
        out_specs=(vmem, vmem),
        scratch_shapes=[
            pltpu.VMEM((128, WIDTH), BF16),
            pltpu.VMEM((128, WIDTH), BF16),
            pltpu.VMEM((128, WIDTH), BF16),
            pltpu.VMEM((8, WIDTH), BF16),
            pltpu.VMEM((8, WIDTH, 256), BF16),
            pltpu.VMEM((8, 256, WIDTH), BF16),
            pltpu.VMEM((32, WIDTH), F32),
            pltpu.VMEM((8, CAP, WIDTH), BF16),
            pltpu.VMEM((7, CAP, WIDTH), BF16),
            pltpu.VMEM((16, CAP, WIDTH), BF16),
            pltpu.VMEM((4, 4, 4, 32, WIDTH), BF16),
            pltpu.VMEM((2, 128, 256), F32),
            pltpu.VMEM((2, 128, 256), F32),
            pltpu.VMEM((2, 128, 256), BF16),
            pltpu.VMEM((4, 4, 4, 32, WIDTH), BF16),
            pltpu.VMEM((4, 3, 4, 32, WIDTH), BF16),
            pltpu.VMEM((4, 4, 32, WIDTH), BF16),
            pltpu.VMEM((4, 7, 16, WIDTH), BF16),
            pltpu.VMEM((16, WIDTH), F32),
            pltpu.VMEM((4, 4, CAP, WIDTH), BF16),
            pltpu.VMEM((16, CAP, WIDTH), BF16),
            pltpu.VMEM((32, WIDTH), F32),
            pltpu.VMEM((8, 8), F32),
            pltpu.VMEM((8, 8), F32),
            pltpu.VMEM((8, 8), F32),
            pltpu.VMEM((3, 8, 8), F32),
            pltpu.VMEM((8, 8), F32),
            pltpu.VMEM((8, 8), F32),
            dma((4,)), dma((3,)), dma((3,)),
            one, dma((4,)), dma((2,)), one,
            dma((4,)), dma((4,)), dma((4,)), dma((4,)), dma((2,)), dma((2,)),
            dma((4,)), dma((4,)), dma((4,)), dma((4,)), one, one,
            dma((3,)), dma((3,)),
        ],
        compiler_params=pltpu.CompilerParams(
            collective_id=0, has_side_effects=True, vmem_limit_bytes=67043328
        ),
    )(
        tokens,
        expert_ids.T,
        router.T,
        w_up.reshape(8, 2, WIDTH, HIDDEN),
        w_down.reshape(HIDDEN, 16 * WIDTH),
        attn_queries.reshape(128, WIDTH),
        attn_keys.reshape(128, WIDTH),
        attn_values.reshape(128, WIDTH),
    )
    return mixed, attended.reshape(1, 128, WIDTH)


def solution(mesh):
    placed = (
        P("dp", "section"),
        P("dp", None),
        P(),
        P("dp", None, "section"),
        P("dp", "section", None),
        P("dp", None, "section"),
        P("dp", None, "section"),
        P("dp", None, "section"),
    )
    return jax.shard_map(
        per_device,
        mesh=mesh,
        in_specs=placed,
        out_specs=(P("dp", "section"), P("dp", None, "section")),
        check_vma=False,
    )
```
